32 devices in a mesh: seq: 8 (over z, y), tensor: 4 (over x, core).
Axes of the slice: x: 2, y: 2, z: 4, core: 2. Of those that a mesh axis runs over, the one named last changes fastest.
Arguments:
- layer_input: bfloat16 [2048, 4096], P('seq', 'tensor'), may hold values from -6 to 6
- norm_gain: float32 [4096], replicated, may hold values from 0.1 to 1.9
- in_weights: bfloat16 [2, 4096, 2048], P(None, None, 'tensor'), may hold values from -0.09375 to 0.09375
- conv_weight: float32 [4, 2048], P(None, 'tensor'), may hold values from -4 to 4
- conv_bias: float32 [2048], P('tensor'), may hold values from -3 to 3
- gate_weights: bfloat16 [2, 8, 256, 256], P(None, 'tensor'), may hold values from -0.375 to 0.375
- gate_bias: float32 [2, 2048], P(None, 'tensor'), may hold values from -4 to 4
- decay_rate: float32 [2048], P('tensor'), may hold values from 1e-06 to 0.03, as said below
- out_weight: bfloat16 [2048, 4096], P('tensor'), may hold values from -0.1875 to 0.1875
- mlp_gain: float32 [4096], replicated, may hold values from 0.1 to 1.9
- mlp_in: bfloat16 [2, 4096, 6144], P(None, 'seq', 'tensor'), may hold values from -0.09375 to 0.09375
- mlp_out: bfloat16 [6144, 4096], P('tensor', 'seq'), may hold values from -0.109375 to 0.109375
Outputs:
- block_output: bfloat16 [2048, 4096], P('seq', 'tensor')
The draws below stay inside these ranges and needn't reach their ends.
Inputs may be any that keep to these rules, and one draw needn't show every extreme that they name: `decay_rate`: every rate is positive.
All inputs are finite; a program needn't handle non-finite values.
Results may differ from the reference program's by a relative error of at most 0.015.
Values may be sent and summed in bfloat16 or wider, within the bound.
A program may use at most 128 MiB of HBM per device.

```python
import jax
import jax.numpy as jnp
from jax import lax

D = 4096
BW = 256
BLOCKS = 8
LRU = 2048
FF = 6144
TAPS = 4
TOKENS = 2048
N_TENSOR = 4


def draw_decay_rate(key, part):
    first_key = jax.random.fold_in(jax.random.fold_in(key, 7103), 0)
    broad = jnp.exp(jax.random.uniform(first_key, (LRU,), jnp.float32, jnp.log(1e-05), jnp.log(0.03)))
    return broad.astype(jnp.float32)


def strengthened(drawn, stream_key, source, target, blocks, factor):
    def block_of(dim):
        return (jnp.arange(drawn.shape[dim]) // (drawn.shape[dim] // blocks)).reshape((-1,) + (1,) * (drawn.ndim - 1 - dim))

    first = jax.random.permutation(stream_key, blocks)[block_of(target)]
    other_side = (block_of(target) + blocks // 2) % blocks
    return jnp.where((block_of(source) == first) | (block_of(source) == other_side), factor * drawn, drawn)


def block_scale(stream_key, shape, pieces, smallest, top_value):
    factor_of = 1.0
    for axis_at, parts in pieces:
        heights = jax.random.uniform(jax.random.fold_in(jax.random.fold_in(stream_key, 6), axis_at), (parts,), jnp.float32, smallest / len(pieces), top_value / len(pieces))
        factor_of = factor_of * jnp.repeat(jnp.exp(heights), shape[axis_at] // parts).reshape((-1,) + (1,) * (len(shape) - 1 - axis_at))
    return factor_of


def bell_draw(stream_key, shape, spread, most, shards=(), held_as=jnp.bfloat16):
    drawn = spread * jax.random.normal(stream_key, shape, jnp.float32)
    if shards:
        drawn = drawn * block_scale(stream_key, shape, shards, -0.22, 0.18)
    return jnp.clip(drawn, -most, most).astype(held_as)


def bell_draw_with(key, shape, width, most, cuts, heavy, dtype=jnp.bfloat16):
    result = width * jax.random.normal(key, shape, jnp.float32)
    if cuts:
        result = result * block_scale(key, shape, cuts, -0.22, 0.18)
    return jnp.clip(strengthened(result, jax.random.fold_in(key, 3), *heavy), -most, most).astype(dtype)


def setup_inputs(seed: int = 0) -> dict:
    keys = jax.random.split(jax.random.key(seed), 13)
    layer_input = bell_draw(keys[0], (TOKENS, D), 1.0, 6.0, ((0, 8), (1, 4)))
    norm_gain = jnp.clip(1.0 + 0.18 * jax.random.normal(keys[1], (D,), jnp.float32), 0.1, 1.9)
    in_weights = bell_draw(keys[2], (2, D, LRU), D ** -0.5, 0.09375, ((2, 4),))
    conv_weight = bell_draw(keys[3], (TAPS, LRU), 1.0, 4.0, ((1, 4),), jnp.float32)
    conv_bias = bell_draw(keys[4], (LRU,), 0.5, 3.0, ((0, 4),), jnp.float32)
    gate_weights = bell_draw(keys[5], (2, BLOCKS, BW, BW), BW ** -0.5, 0.375, ((1, 4),))
    gate_bias = bell_draw(keys[6], (2, LRU), 1.0, 4.0, ((1, 4),), jnp.float32)
    decay_rate = draw_decay_rate(jax.random.fold_in(keys[12], 71), 0)
    out_weight = bell_draw_with(keys[8], (LRU, D), LRU ** -0.5, 0.1875, ((0, 4),), (0, 1, 4, 2.0))
    mlp_gain = jnp.clip(1.0 + 0.18 * jax.random.normal(keys[9], (D,), jnp.float32), 0.1, 1.9)
    mlp_in = bell_draw(keys[10], (2, D, FF), D ** -0.5, 0.09375, ((1, 8), (2, 4)))
    mlp_out = bell_draw_with(keys[11], (FF, D), FF ** -0.5, 0.109375, ((0, 4), (1, 8)), (0, 1, 8, 2.0))
    return dict(layer_input=layer_input, norm_gain=norm_gain, in_weights=in_weights, conv_weight=conv_weight, conv_bias=conv_bias, gate_weights=gate_weights, gate_bias=gate_bias, decay_rate=decay_rate, out_weight=out_weight, mlp_gain=mlp_gain, mlp_in=mlp_in, mlp_out=mlp_out)


def rms_scale(rows, gain):
    values = rows.astype(jnp.float32)
    mean_square = lax.optimization_barrier(jnp.mean(values * values, axis=-1, keepdims=True))
    return (values * lax.rsqrt(mean_square + 1e-06) * gain).astype(jnp.bfloat16)

def advance(state, inputs):
    decay, driven = inputs
    state = decay * state + driven
    return (state, state)

def reference(layer_input, norm_gain, in_weights, conv_weight, conv_bias, gate_weights, gate_bias, decay_rate, out_weight, mlp_gain, mlp_in, mlp_out):
    normed = rms_scale(layer_input, norm_gain)
    branch_x = jnp.dot(normed, in_weights[0], preferred_element_type=jnp.float32).astype(jnp.bfloat16)
    branch_y = jax.nn.gelu(jnp.dot(normed, in_weights[1], preferred_element_type=jnp.float32), approximate=True)
    padded = jnp.concatenate([jnp.zeros((TAPS - 1, LRU), jnp.bfloat16), branch_x], axis=0).astype(jnp.float32)
    convolved = jnp.zeros((TOKENS, LRU), jnp.float32) + conv_bias
    for tap_index in range(TAPS):
        start_row = TAPS - 1 - tap_index
        convolved = convolved + conv_weight[tap_index] * padded[start_row:start_row + TOKENS]
    conv_out = convolved.astype(jnp.bfloat16)
    blocks_in = conv_out.astype(jnp.float32).reshape(TOKENS, BLOCKS, BW)
    gate_pre = jnp.einsum('tnc,knce->ktne', blocks_in, gate_weights.astype(jnp.float32)).reshape(2, TOKENS, LRU) + gate_bias[:, None, :]
    log_decay = -8.0 * jax.nn.sigmoid(gate_pre[0]) * decay_rate
    decay = jnp.exp(log_decay)
    driven = conv_out.astype(jnp.float32) * jax.nn.sigmoid(gate_pre[1]) * jnp.sqrt(-jnp.expm1(2.0 * log_decay))
    _, states = lax.scan(advance, jnp.zeros((LRU,), jnp.float32), (decay, driven))
    mixed = (states * branch_y).astype(jnp.bfloat16)
    group = LRU // N_TENSOR
    rec_sum = jnp.zeros((TOKENS, D), jnp.float32)
    for group_index in range(N_TENSOR):
        term = jnp.dot(mixed[:, group_index * group:(group_index + 1) * group], out_weight[group_index * group:(group_index + 1) * group], preferred_element_type=jnp.float32).astype(jnp.bfloat16)
        term = lax.optimization_barrier(term)
        rec_sum = rec_sum + term.astype(jnp.float32)
    residual = (layer_input.astype(jnp.float32) + rec_sum).astype(jnp.bfloat16)
    mlp_normed = rms_scale(residual, mlp_gain)
    gate = jnp.dot(mlp_normed, mlp_in[0], preferred_element_type=jnp.float32)
    upward = jnp.dot(mlp_normed, mlp_in[1], preferred_element_type=jnp.float32)
    hidden = (jax.nn.gelu(gate, approximate=True) * upward).astype(jnp.bfloat16)
    down = jnp.dot(hidden, mlp_out, preferred_element_type=jnp.float32)
    return (residual.astype(jnp.float32) + down).astype(jnp.bfloat16)
```

```python
import jax
import jax.numpy as jnp
from jax import lax
from jax.experimental import pallas as pl
from jax.experimental.pallas import tpu as pltpu
from jax.sharding import PartitionSpec as P

CORES = 2
F32 = jnp.float32
BF16 = jnp.bfloat16


def shifted(value, axis, steps):
    count = lax.axis_size(axis)
    return lax.ppermute(value, axis, [(i, i + steps) for i in range(count - steps)])


def core_swap(value):
    count = lax.axis_size("tensor")
    return lax.ppermute(value, "tensor", [(i, i ^ 1) for i in range(count)])


def chip_shift(value, steps):
    count = lax.axis_size("tensor")
    return lax.ppermute(
        value, "tensor", [(i, (i + CORES * steps) % count) for i in range(count)]
    )


def pick(stacked, index):
    return lax.dynamic_index_in_dim(stacked, index, 0, keepdims=False)


def gather_tensor(block):
    count = lax.axis_size("tensor")
    chips = count // CORES
    here = lax.axis_index("tensor")
    chip, core = here // CORES, here % CORES
    pieces = []
    received = [block] + [chip_shift(block, k) for k in range(1, chips)]
    for part in received:
        pieces += [part, core_swap(part)]
    stacked = jnp.stack(pieces)
    return [
        pick(stacked, lax.rem(chip - t // CORES + chips, chips) * CORES + (core ^ (t % CORES)))
        for t in range(count)
    ]


def scatter_tensor(partial):
    count = lax.axis_size("tensor")
    chips = count // CORES
    here = lax.axis_index("tensor")
    chip, core = here // CORES, here % CORES
    rows, columns = partial.shape
    width = columns // count

    def block(t):
        return lax.dynamic_slice_in_dim(partial, t * width, width, 1)

    to_chip = [lax.rem(chip + k, chips) for k in range(chips)]
    order = list(range(1, chips)) + [0]
    sums = {}
    for k in order:
        other = core_swap(block(to_chip[k] * CORES + (1 - core)).astype(BF16))
        sums[k] = block(to_chip[k] * CORES + core).astype(F32) + other.astype(F32)
    total = sums[0]
    for k in range(1, chips):
        total = total + chip_shift(sums[k].astype(BF16), k).astype(F32)
    return total


def square_size(count):
    return 4 if count % 4 == 0 else 1


def square_swap(value, offset):
    if offset == 0:
        return value
    count = lax.axis_size("seq")
    return lax.ppermute(value, "seq", [(i, i ^ offset) for i in range(count)])


def gather_far(weight):
    count = lax.axis_size("seq")
    size = square_size(count)
    far = count // size
    here = lax.axis_index("seq") // size
    parts = [weight]
    for k in range(1, far):
        parts.append(
            lax.ppermute(weight, "seq", [(i, (i + k * size) % count) for i in range(count)])
        )
    if far == 1:
        return parts
    if far == 2:
        first = here == 0
        return [jnp.where(first, parts[0], parts[1]), jnp.where(first, parts[1], parts[0])]
    stacked = jnp.stack(parts)
    return [pick(stacked, lax.rem(here - q + far, far)) for q in range(far)]


def expm1_neg(y):
    series = jnp.ones_like(y)
    for n in range(10, 1, -1):
        series = 1.0 + series * y * (1.0 / n)
    return jnp.where(y > -0.5, -y * series, 1.0 - jnp.exp(y))


def recurrence_kernel(x_ref, rim_ref, cw_ref, cb_ref, gw_ref, gb_ref, rate_ref, a_ref, b_ref):
    rows, width = x_ref.shape
    pad = rim_ref.shape[0]
    padded = jnp.concatenate([rim_ref[...].astype(F32), x_ref[...].astype(F32)], axis=0)
    conv = jnp.zeros((rows, width), F32) + cb_ref[...]
    for tap in range(cw_ref.shape[0]):
        conv = conv + cw_ref[tap : tap + 1, :] * padded[pad - tap : pad - tap + rows]
    conv_bf = conv.astype(BF16)
    conv_f = conv_bf.astype(F32)
    blocks, bw = gw_ref.shape[1], gw_ref.shape[2]
    index = lax.broadcasted_iota(jnp.int32, (rows, bw), 0)
    for n in range(blocks):
        cols = slice(n * bw, (n + 1) * bw)
        inp = conv_bf[:, cols]
        gate0 = jnp.dot(inp, gw_ref[0, n], preferred_element_type=F32) + gb_ref[0:1, cols]
        gate1 = jnp.dot(inp, gw_ref[1, n], preferred_element_type=F32) + gb_ref[1:2, cols]
        log_decay = -8.0 * jax.nn.sigmoid(gate0) * rate_ref[0:1, cols]
        a = jnp.exp(log_decay)
        b = conv_f[:, cols] * jax.nn.sigmoid(gate1) * jnp.sqrt(expm1_neg(2.0 * log_decay))
        step = 1
        while step < rows:
            valid = index >= step
            before_a = jnp.where(valid, pltpu.roll(a, step, 0), 1.0)
            before_b = jnp.where(valid, pltpu.roll(b, step, 0), 0.0)
            b = a * before_b + b
            a = a * before_a
            step *= 2
        a_ref[:, cols] = a
        b_ref[:, cols] = b


def recurrence(branch_x, rim, conv_weight, conv_bias, gate_weights, gate_bias, decay_rate):
    shape = jax.ShapeDtypeStruct(branch_x.shape, F32)
    return pl.pallas_call(
        recurrence_kernel,
        out_shape=(shape, shape),
        in_specs=[pl.BlockSpec(memory_space=pltpu.VMEM)] * 7,
        out_specs=(pl.BlockSpec(memory_space=pltpu.VMEM),) * 2,
        compiler_params=pltpu.CompilerParams(vmem_limit_bytes=24 * 1024 * 1024),
        cost_estimate=pl.CostEstimate(
            flops=8_000_000_000, bytes_accessed=3_000_000, transcendentals=0
        ),
    )(branch_x, rim, conv_weight, conv_bias[None], gate_weights, gate_bias, decay_rate[None])


def entering_state(a, b):
    count = lax.axis_size("seq")
    pair = jnp.stack([a, b])
    one, two = shifted(pair, "seq", 1), shifted(pair, "seq", 2)
    a, b = one[0] * two[0], one[0] * two[1] + one[1]
    step = 2
    while step < count:
        got = shifted(jnp.stack([a, b]), "seq", step)
        a, b = a * got[0], a * got[1] + b
        step *= 2
    return b


def shards(
    layer_input,
    norm_gain,
    in_weights,
    conv_weight,
    conv_bias,
    gate_weights,
    gate_bias,
    decay_rate,
    out_weight,
    mlp_gain,
    mlp_in,
    mlp_out,
):
    rows, own_width = layer_input.shape
    seq_count = lax.axis_size("seq")
    size = square_size(seq_count)
    far = seq_count // size
    seq_here = lax.axis_index("seq")
    place = seq_here % size
    tensor_here = lax.axis_index("tensor")

    up_weights = gather_far(mlp_in)
    down_weights = gather_far(mlp_out)

    blocks = gather_tensor(layer_input)
    whole = jnp.concatenate(blocks, axis=1)
    values = whole.astype(F32)
    scale = lax.rsqrt(jnp.mean(values * values, axis=-1, keepdims=True) + 1e-06)
    normed = (values * scale * norm_gain).astype(BF16)
    branch_x = jnp.dot(normed, in_weights[0], preferred_element_type=F32).astype(BF16)
    rim_rows = 8
    rim = shifted(branch_x[rows - rim_rows :], "seq", 1)
    branch_y = jax.nn.gelu(
        jnp.dot(normed, in_weights[1], preferred_element_type=F32), approximate=True
    )
    cum_decay, cum_state = recurrence(
        branch_x, rim, conv_weight, conv_bias, gate_weights, gate_bias, decay_rate
    )
    carried = entering_state(cum_decay[-1], cum_state[-1])
    mixed = ((cum_decay * carried + cum_state) * branch_y).astype(BF16)
    partial = jnp.dot(mixed, out_weight, preferred_element_type=F32).astype(BF16)
    residual = (layer_input.astype(F32) + scatter_tensor(partial)).astype(BF16)
    res = residual.astype(F32)
    own_gain = lax.dynamic_slice_in_dim(mlp_gain, tensor_here * own_width, own_width, 0)
    gained = (res * own_gain).astype(BF16)
    squares = jnp.sum(res * res, axis=-1)
    width_all = mlp_gain.shape[0]

    mids = jnp.concatenate(gather_tensor(gained), axis=1)
    squares = squares + core_swap(squares)
    chips = lax.axis_size("tensor") // CORES
    squares = squares + sum(chip_shift(squares, k) for k in range(1, chips))
    mlp_scale = lax.rsqrt(squares / width_all + 1e-06)[:, None]

    piece = width_all // seq_count
    halves = mlp_in.shape[0]
    feed = jnp.concatenate(up_weights, axis=1)

    def columns_for(where):
        return jnp.concatenate(
            [
                lax.dynamic_slice_in_dim(mids, (q * size + where) * piece, piece, 1)
                for q in range(far)
            ],
            axis=1,
        )

    offsets = list(range(size - 1, -1, -1))
    tokens = {o: square_swap(columns_for(place ^ o), o) for o in offsets}
    gate_up = [jnp.zeros((rows, mlp_in.shape[2]), F32) for _ in range(halves)]
    for o in offsets:
        for half in range(halves):
            term = jnp.dot(tokens[o], feed[half], preferred_element_type=F32)
            if o:
                term = square_swap(term.astype(BF16), o).astype(F32)
            gate_up[half] = gate_up[half] + term
    gate = gate_up[0] * mlp_scale
    hidden = (jax.nn.gelu(gate, approximate=True) * (gate_up[1] * mlp_scale)).astype(BF16)

    down_w = jnp.concatenate(down_weights, axis=1)
    back = {}
    for o in offsets:
        term = jnp.dot(square_swap(hidden, o), down_w, preferred_element_type=F32)
        back[o] = square_swap(term.astype(BF16), o)
    stacked = jnp.stack([back[o] for o in range(size)])
    ordered = [pick(stacked, place ^ r) for r in range(size)]
    down = jnp.concatenate(
        [
            ordered[r][:, q * piece : (q + 1) * piece]
            for q in range(far)
            for r in range(size)
        ],
        axis=1,
    )
    return (res + scatter_tensor(down)).astype(BF16)


def solution(mesh):
    return jax.shard_map(
        shards,
        mesh=mesh,
        in_specs=(
            P("seq", "tensor"),
            P(),
            P(None, None, "tensor"),
            P(None, "tensor"),
            P("tensor"),
            P(None, "tensor", None, None),
            P(None, "tensor"),
            P("tensor"),
            P("tensor", None),
            P(),
            P(None, "seq", "tensor"),
            P("tensor", "seq"),
        ),
        out_specs=P("seq", "tensor"),
        check_vma=False,
    )
```

```python
import jax
import jax.numpy as jnp
from jax import lax
from jax.experimental import pallas as pl
from jax.experimental.pallas import tpu as pltpu
from jax.sharding import PartitionSpec as P

CORES = 2
F32 = jnp.float32
BF16 = jnp.bfloat16


def shifted(value, axis, steps):
    count = lax.axis_size(axis)
    return lax.ppermute(value, axis, [(i, i + steps) for i in range(count - steps)])


def core_swap(value):
    count = lax.axis_size("tensor")
    return lax.ppermute(value, "tensor", [(i, i ^ 1) for i in range(count)])


def chip_shift(value, steps):
    count = lax.axis_size("tensor")
    return lax.ppermute(
        value, "tensor", [(i, (i + CORES * steps) % count) for i in range(count)]
    )


def pick(stacked, index):
    return lax.dynamic_index_in_dim(stacked, index, 0, keepdims=False)


def gather_tensor(block):
    count = lax.axis_size("tensor")
    chips = count // CORES
    here = lax.axis_index("tensor")
    chip, core = here // CORES, here % CORES
    pieces = []
    received = [block] + [chip_shift(block, k) for k in range(1, chips)]
    for part in received:
        pieces += [part, core_swap(part)]
    stacked = jnp.stack(pieces)
    return [
        pick(stacked, lax.rem(chip - t // CORES + chips, chips) * CORES + (core ^ (t % CORES)))
        for t in range(count)
    ]


def scatter_tensor(partial):
    count = lax.axis_size("tensor")
    chips = count // CORES
    here = lax.axis_index("tensor")
    chip, core = here // CORES, here % CORES
    rows, columns = partial.shape
    width = columns // count

    def block(t):
        return lax.dynamic_slice_in_dim(partial, t * width, width, 1)

    to_chip = [lax.rem(chip + k, chips) for k in range(chips)]
    order = list(range(1, chips)) + [0]
    sums = {}
    for k in order:
        other = core_swap(block(to_chip[k] * CORES + (1 - core)).astype(BF16))
        sums[k] = block(to_chip[k] * CORES + core).astype(F32) + other.astype(F32)
    total = sums[0]
    for k in range(1, chips):
        total = total + chip_shift(sums[k].astype(BF16), k).astype(F32)
    return total


def square_size(count):
    return 4 if count % 4 == 0 else 1


def square_swap(value, offset):
    if offset == 0:
        return value
    count = lax.axis_size("seq")
    return lax.ppermute(value, "seq", [(i, i ^ offset) for i in range(count)])


def gather_far(weight, axis):
    count = lax.axis_size("seq")
    size = square_size(count)
    if count == size:
        return weight
    groups = [list(range(r, count, size)) for r in range(size)]
    return lax.all_gather(weight, "seq", axis=axis, tiled=True, axis_index_groups=groups)


def direct(value, pairs):
    count = lax.axis_size("tensor")
    return lax.ppermute(
        value, ("seq", "tensor"), [(a * count + b, c * count + d) for (a, b), (c, d) in pairs]
    )


def plane_routes(offset):
    routes = []
    for s in range(lax.axis_size("seq")):
        for x in range(CORES):
            holder = (s, x * CORES + x)
            owner = (s ^ offset, x * CORES + (s % 4) // 2)
            if holder != owner:
                routes.append((holder, owner))
    return routes


def across_chips(keeper):
    pairs = []
    for s in range(lax.axis_size("seq")):
        for x in range(CORES):
            giver = ((s, x * CORES + 1 - x), (s, (1 - x) * CORES + 1 - x))
            pairs.append(giver if keeper else giver[::-1])
    return pairs


def spread_columns(gained, piece):
    place = lax.axis_index("seq") % 4
    here = lax.axis_index("tensor")
    chip, core = here // CORES, here % CORES
    got = []
    for o in range(4):
        block = lax.dynamic_slice_in_dim(gained, ((place ^ o) % 2) * piece, piece, 1)
        moved = direct(block, [(owner, holder) for holder, owner in plane_routes(o)])
        if o == 0:
            moved = jnp.where(place // 2 == core, block, moved)
        got.append(moved)
    held = jnp.concatenate(got, axis=0)
    passed = direct(held, across_chips(False))
    mine = jnp.where(chip == core, held, passed)
    other = core_swap(mine)
    first = core == 0
    return jnp.where(first, mine, other), jnp.where(first, other, mine)


def collect_columns(terms, piece):
    place = lax.axis_index("seq") % 4
    here = lax.axis_index("tensor")
    chip, core = here // CORES, here % CORES
    low, high = terms[:, :piece], terms[:, piece:]
    first = core == 0
    mine = jnp.where(first, low, high)
    mine = mine + core_swap(jnp.where(first, high, low).astype(BF16)).astype(F32)
    total = (mine + direct(mine.astype(BF16), across_chips(True)).astype(F32)).astype(BF16)
    rows = total.shape[0] // 4
    got = []
    for o in range(4):
        block = total[o * rows : (o + 1) * rows]
        moved = direct(block, plane_routes(o))
        if o == 0:
            moved = jnp.where(chip == core, block, moved)
        got.append(moved)
    stacked = jnp.stack(got)
    turn = ((place // 2) ^ core) * 2
    return jnp.concatenate([pick(stacked, turn + (k ^ (place % 2))) for k in range(2)], axis=1)


def expm1_neg(y):
    series = jnp.ones_like(y)
    for n in range(10, 1, -1):
        series = 1.0 + series * y * (1.0 / n)
    return jnp.where(y > -0.5, -y * series, 1.0 - jnp.exp(y))


def recurrence_kernel(x_ref, rim_ref, cw_ref, cb_ref, gw_ref, gb_ref, rate_ref, a_ref, b_ref):
    rows, width = x_ref.shape
    pad = rim_ref.shape[0]
    padded = jnp.concatenate([rim_ref[...].astype(F32), x_ref[...].astype(F32)], axis=0)
    conv = jnp.zeros((rows, width), F32) + cb_ref[...]
    for tap in range(cw_ref.shape[0]):
        conv = conv + cw_ref[tap : tap + 1, :] * padded[pad - tap : pad - tap + rows]
    conv_bf = conv.astype(BF16)
    conv_f = conv_bf.astype(F32)
    blocks, bw = gw_ref.shape[1], gw_ref.shape[2]
    index = lax.broadcasted_iota(jnp.int32, (rows, bw), 0)
    for n in range(blocks):
        cols = slice(n * bw, (n + 1) * bw)
        inp = conv_bf[:, cols]
        gate0 = jnp.dot(inp, gw_ref[0, n], preferred_element_type=F32) + gb_ref[0:1, cols]
        gate1 = jnp.dot(inp, gw_ref[1, n], preferred_element_type=F32) + gb_ref[1:2, cols]
        log_decay = -8.0 * jax.nn.sigmoid(gate0) * rate_ref[0:1, cols]
        a = jnp.exp(log_decay)
        b = conv_f[:, cols] * jax.nn.sigmoid(gate1) * jnp.sqrt(expm1_neg(2.0 * log_decay))
        step = 1
        while step < rows:
            valid = index >= step
            before_a = jnp.where(valid, pltpu.roll(a, step, 0), 1.0)
            before_b = jnp.where(valid, pltpu.roll(b, step, 0), 0.0)
            b = a * before_b + b
            a = a * before_a
            step *= 2
        a_ref[:, cols] = a
        b_ref[:, cols] = b


def recurrence(branch_x, rim, conv_weight, conv_bias, gate_weights, gate_bias, decay_rate):
    shape = jax.ShapeDtypeStruct(branch_x.shape, F32)
    return pl.pallas_call(
        recurrence_kernel,
        out_shape=(shape, shape),
        in_specs=[pl.BlockSpec(memory_space=pltpu.VMEM)] * 7,
        out_specs=(pl.BlockSpec(memory_space=pltpu.VMEM),) * 2,
        compiler_params=pltpu.CompilerParams(vmem_limit_bytes=24 * 1024 * 1024),
        cost_estimate=pl.CostEstimate(
            flops=8_000_000_000, bytes_accessed=3_000_000, transcendentals=0
        ),
    )(branch_x, rim, conv_weight, conv_bias[None], gate_weights, gate_bias, decay_rate[None])


def entering_state(a, b):
    count = lax.axis_size("seq")
    pair = jnp.stack([a, b])
    one, two = shifted(pair, "seq", 1), shifted(pair, "seq", 2)
    a, b = one[0] * two[0], one[0] * two[1] + one[1]
    step = 2
    while step < count:
        got = shifted(jnp.stack([a, b]), "seq", step)
        a, b = a * got[0], a * got[1] + b
        step *= 2
    return b


def shards(
    layer_input,
    norm_gain,
    in_weights,
    conv_weight,
    conv_bias,
    gate_weights,
    gate_bias,
    decay_rate,
    out_weight,
    mlp_gain,
    mlp_in,
    mlp_out,
):
    rows, own_width = layer_input.shape
    seq_count = lax.axis_size("seq")
    size = square_size(seq_count)
    far = seq_count // size
    seq_here = lax.axis_index("seq")
    place = seq_here % size
    tensor_here = lax.axis_index("tensor")

    halves = mlp_in.shape[0]
    feed = [gather_far(mlp_in[half], 0) for half in range(halves)]
    down_w = gather_far(mlp_out, 1)

    blocks = gather_tensor(layer_input)
    whole = jnp.concatenate(blocks, axis=1)
    values = whole.astype(F32)
    scale = lax.rsqrt(jnp.mean(values * values, axis=-1, keepdims=True) + 1e-06)
    normed = (values * scale * norm_gain).astype(BF16)
    branch_x = jnp.dot(normed, in_weights[0], preferred_element_type=F32).astype(BF16)
    rim_rows = 8
    rim = shifted(branch_x[rows - rim_rows :], "seq", 1)
    branch_y = jax.nn.gelu(
        jnp.dot(normed, in_weights[1], preferred_element_type=F32), approximate=True
    )
    cum_decay, cum_state = recurrence(
        branch_x, rim, conv_weight, conv_bias, gate_weights, gate_bias, decay_rate
    )
    carried = entering_state(cum_decay[-1], cum_state[-1])
    mixed = ((cum_decay * carried + cum_state) * branch_y).astype(BF16)
    partial = jnp.dot(mixed, out_weight, preferred_element_type=F32).astype(BF16)
    residual = (layer_input.astype(F32) + scatter_tensor(partial)).astype(BF16)
    res = residual.astype(F32)
    own_gain = lax.dynamic_slice_in_dim(mlp_gain, tensor_here * own_width, own_width, 0)
    gained = (res * own_gain).astype(BF16)
    squares = jnp.sum(res * res, axis=-1)
    width_all = mlp_gain.shape[0]

    squares = squares + core_swap(squares)
    chips = lax.axis_size("tensor") // CORES
    squares = squares + sum(chip_shift(squares, k) for k in range(1, chips))
    mlp_scale = lax.rsqrt(squares / width_all + 1e-06)[:, None]

    piece = width_all // seq_count
    short = size == 4 and far == CORES and lax.axis_size("tensor") == CORES * CORES
    short = short and own_width == 2 * piece
    offsets = list(range(size - 1, -1, -1))
    if short:
        low, high = spread_columns(gained, piece)
        tokens = {
            o: jnp.concatenate(
                [low[o * rows : (o + 1) * rows], high[o * rows : (o + 1) * rows]], axis=1
            )
            for o in offsets
        }
    else:
        mids = jnp.concatenate(gather_tensor(gained), axis=1)
        wide = mids.reshape(rows, far, size, piece)

        def columns_for(where):
            return lax.dynamic_index_in_dim(wide, where, 2, keepdims=False).reshape(
                rows, far * piece
            )

        tokens = {o: square_swap(columns_for(place ^ o), o) for o in offsets}
    gate_up = []
    for half in range(halves):
        total = jnp.zeros((rows, mlp_in.shape[2]), F32)
        for o in offsets:
            term = jnp.dot(tokens[o], feed[half], preferred_element_type=F32)
            if o:
                term = square_swap(term.astype(BF16), o).astype(F32)
            total = total + term
        gate_up.append(total)
    gate = gate_up[0] * mlp_scale
    hidden = (jax.nn.gelu(gate, approximate=True) * (gate_up[1] * mlp_scale)).astype(BF16)

    spread = {o: square_swap(hidden, o) for o in offsets}
    if short:
        terms = jnp.concatenate(
            [jnp.dot(spread[o], down_w, preferred_element_type=F32) for o in range(size)], axis=0
        )
        return (res + collect_columns(terms, piece).astype(F32)).astype(BF16)
    back = {}
    for o in offsets:
        term = jnp.dot(spread[o], down_w, preferred_element_type=F32)
        back[o] = square_swap(term.astype(BF16), o)
    stacked = jnp.stack([back[o] for o in range(size)])
    ordered = [pick(stacked, place ^ r) for r in range(size)]
    down = jnp.concatenate(
        [ordered[r][:, q * piece : (q + 1) * piece] for q in range(far) for r in range(size)],
        axis=1,
    )
    return (res + scatter_tensor(down)).astype(BF16)


def solution(mesh):
    return jax.shard_map(
        shards,
        mesh=mesh,
        in_specs=(
            P("seq", "tensor"),
            P(),
            P(None, None, "tensor"),
            P(None, "tensor"),
            P("tensor"),
            P(None, "tensor", None, None),
            P(None, "tensor"),
            P("tensor"),
            P("tensor", None),
            P(),
            P(None, "seq", "tensor"),
            P("tensor", "seq"),
        ),
        out_specs=P("seq", "tensor"),
        check_vma=False,
    )
```

```python
import jax
import jax.numpy as jnp
from jax import lax
from jax.experimental import pallas as pl
from jax.experimental.pallas import tpu as pltpu
from jax.sharding import PartitionSpec as P

CORES = 2
F32 = jnp.float32
BF16 = jnp.bfloat16


def shifted(value, axis, steps):
    count = lax.axis_size(axis)
    return lax.ppermute(value, axis, [(i, i + steps) for i in range(count - steps)])


def core_swap(value):
    count = lax.axis_size("tensor")
    return lax.ppermute(value, "tensor", [(i, i ^ 1) for i in range(count)])


def chip_shift(value, steps):
    count = lax.axis_size("tensor")
    return lax.ppermute(
        value, "tensor", [(i, (i + CORES * steps) % count) for i in range(count)]
    )


def pick(stacked, index):
    return lax.dynamic_index_in_dim(stacked, index, 0, keepdims=False)


def gather_tensor(block):
    count = lax.axis_size("tensor")
    chips = count // CORES
    here = lax.axis_index("tensor")
    chip, core = here // CORES, here % CORES
    pieces = []
    received = [block] + [chip_shift(block, k) for k in range(1, chips)]
    for part in received:
        pieces += [part, core_swap(part)]
    stacked = jnp.stack(pieces)
    return [
        pick(stacked, lax.rem(chip - t // CORES + chips, chips) * CORES + (core ^ (t % CORES)))
        for t in range(count)
    ]


def scatter_tensor(partial):
    count = lax.axis_size("tensor")
    chips = count // CORES
    here = lax.axis_index("tensor")
    chip, core = here // CORES, here % CORES
    rows, columns = partial.shape
    width = columns // count

    def block(t):
        return lax.dynamic_slice_in_dim(partial, t * width, width, 1)

    to_chip = [lax.rem(chip + k, chips) for k in range(chips)]
    order = list(range(1, chips)) + [0]
    sums = {}
    for k in order:
        other = core_swap(block(to_chip[k] * CORES + (1 - core)).astype(BF16))
        sums[k] = block(to_chip[k] * CORES + core).astype(F32) + other.astype(F32)
    total = sums[0]
    for k in range(1, chips):
        total = total + chip_shift(sums[k].astype(BF16), k).astype(F32)
    return total


def square_size(count):
    return 4 if count % 4 == 0 else 1


def square_swap(value, offset):
    if offset == 0:
        return value
    count = lax.axis_size("seq")
    return lax.ppermute(value, "seq", [(i, i ^ offset) for i in range(count)])


def gather_far(weight, axis):
    count = lax.axis_size("seq")
    size = square_size(count)
    if count == size:
        return weight
    groups = [list(range(r, count, size)) for r in range(size)]
    return lax.all_gather(weight, "seq", axis=axis, tiled=True, axis_index_groups=groups)


def direct(value, pairs):
    count = lax.axis_size("tensor")
    return lax.ppermute(
        value, ("seq", "tensor"), [(a * count + b, c * count + d) for (a, b), (c, d) in pairs]
    )


def plane_routes(offset):
    routes = []
    for s in range(lax.axis_size("seq")):
        for x in range(CORES):
            holder = (s, x * CORES + x)
            owner = (s ^ offset, x * CORES + (s % 4) // 2)
            if holder != owner:
                routes.append((holder, owner))
    return routes


def across_chips(keeper):
    pairs = []
    for s in range(lax.axis_size("seq")):
        for x in range(CORES):
            giver = ((s, x * CORES + 1 - x), (s, (1 - x) * CORES + 1 - x))
            pairs.append(giver if keeper else giver[::-1])
    return pairs


def spread_columns(gained, piece):
    place = lax.axis_index("seq") % 4
    here = lax.axis_index("tensor")
    chip, core = here // CORES, here % CORES
    got = []
    for o in range(4):
        block = lax.dynamic_slice_in_dim(gained, ((place ^ o) % 2) * piece, piece, 1)
        moved = direct(block, [(owner, holder) for holder, owner in plane_routes(o)])
        if o == 0:
            moved = jnp.where(place // 2 == core, block, moved)
        got.append(moved)
    held = jnp.concatenate(got, axis=0)
    passed = direct(held, across_chips(False))
    mine = jnp.where(chip == core, held, passed)
    other = core_swap(mine)
    first = core == 0
    return jnp.where(first, mine, other), jnp.where(first, other, mine)


def collect_columns(terms, piece):
    place = lax.axis_index("seq") % 4
    here = lax.axis_index("tensor")
    chip, core = here // CORES, here % CORES
    low, high = terms[:, :piece], terms[:, piece:]
    first = core == 0
    mine = jnp.where(first, low, high)
    mine = mine + core_swap(jnp.where(first, high, low).astype(BF16)).astype(F32)
    total = (mine + direct(mine.astype(BF16), across_chips(True)).astype(F32)).astype(BF16)
    rows = total.shape[0] // 4
    got = []
    for o in range(4):
        block = total[o * rows : (o + 1) * rows]
        moved = direct(block, plane_routes(o))
        if o == 0:
            moved = jnp.where(chip == core, block, moved)
        got.append(moved)
    stacked = jnp.stack(got)
    turn = ((place // 2) ^ core) * 2
    return jnp.concatenate([pick(stacked, turn + (k ^ (place % 2))) for k in range(2)], axis=1)


def expm1_neg(y):
    series = jnp.ones_like(y)
    for n in range(10, 1, -1):
        series = 1.0 + series * y * (1.0 / n)
    return jnp.where(y > -0.5, -y * series, 1.0 - jnp.exp(y))


def recurrence_kernel(x_ref, rim_ref, cw_ref, cb_ref, gw_ref, gb_ref, rate_ref, a_ref, b_ref):
    rows, width = x_ref.shape
    pad = rim_ref.shape[0]
    padded = jnp.concatenate([rim_ref[...].astype(F32), x_ref[...].astype(F32)], axis=0)
    conv = jnp.zeros((rows, width), F32) + cb_ref[...]
    for tap in range(cw_ref.shape[0]):
        conv = conv + cw_ref[tap : tap + 1, :] * padded[pad - tap : pad - tap + rows]
    conv_bf = conv.astype(BF16)
    conv_f = conv_bf.astype(F32)
    blocks, bw = gw_ref.shape[1], gw_ref.shape[2]
    index = lax.broadcasted_iota(jnp.int32, (rows, bw), 0)
    for n in range(blocks):
        cols = slice(n * bw, (n + 1) * bw)
        inp = conv_bf[:, cols]
        gate0 = jnp.dot(inp, gw_ref[0, n], preferred_element_type=F32) + gb_ref[0:1, cols]
        gate1 = jnp.dot(inp, gw_ref[1, n], preferred_element_type=F32) + gb_ref[1:2, cols]
        log_decay = -8.0 * jax.nn.sigmoid(gate0) * rate_ref[0:1, cols]
        a = jnp.exp(log_decay)
        b = conv_f[:, cols] * jax.nn.sigmoid(gate1) * jnp.sqrt(expm1_neg(2.0 * log_decay))
        step = 1
        while step < rows:
            valid = index >= step
            before_a = jnp.where(valid, pltpu.roll(a, step, 0), 1.0)
            before_b = jnp.where(valid, pltpu.roll(b, step, 0), 0.0)
            b = a * before_b + b
            a = a * before_a
            step *= 2
        a_ref[:, cols] = a
        b_ref[:, cols] = b


def recurrence(branch_x, rim, conv_weight, conv_bias, gate_weights, gate_bias, decay_rate):
    shape = jax.ShapeDtypeStruct(branch_x.shape, F32)
    return pl.pallas_call(
        recurrence_kernel,
        out_shape=(shape, shape),
        in_specs=[pl.BlockSpec(memory_space=pltpu.VMEM)] * 7,
        out_specs=(pl.BlockSpec(memory_space=pltpu.VMEM),) * 2,
        compiler_params=pltpu.CompilerParams(vmem_limit_bytes=24 * 1024 * 1024),
        cost_estimate=pl.CostEstimate(
            flops=8_000_000_000, bytes_accessed=3_000_000, transcendentals=0
        ),
    )(branch_x, rim, conv_weight, conv_bias[None], gate_weights, gate_bias, decay_rate[None])


def prefix_kernel(count, pair_ref, out_ref, slots, send_sem, recv_sem):
    me = lax.axis_index("seq")
    barrier = pltpu.get_barrier_semaphore()
    for k in range(1, count):
        pl.semaphore_signal(
            barrier,
            inc=1,
            device_id={"seq": lax.rem(me + k, count)},
            device_id_type=pl.DeviceIdType.MESH,
        )
    pl.semaphore_wait(barrier, count - 1)
    copies = []
    for k in range(1, count):
        copy = pltpu.make_async_remote_copy(
            src_ref=pair_ref,
            dst_ref=slots.at[k],
            send_sem=send_sem.at[k],
            recv_sem=recv_sem.at[k],
            device_id={"seq": lax.rem(me + k, count)},
            device_id_type=pl.DeviceIdType.MESH,
        )
        copy.start()
        copies.append(copy)
    for copy in copies:
        copy.wait()
    state = jnp.zeros(out_ref.shape, F32)
    for k in range(count - 1, 0, -1):
        later = slots[k, 0:1, :] * state + slots[k, 1:2, :]
        state = jnp.where(me >= k, later, state)
    out_ref[...] = state


def entering_state(a, b):
    count = lax.axis_size("seq")
    rows = 8
    pair = jnp.concatenate([a[None], b[None], jnp.zeros((rows - 2, a.shape[0]), F32)], axis=0)
    return pl.pallas_call(
        lambda *refs: prefix_kernel(count, *refs),
        out_shape=jax.ShapeDtypeStruct((1, a.shape[0]), F32),
        in_specs=[pl.BlockSpec(memory_space=pltpu.VMEM)],
        out_specs=pl.BlockSpec(memory_space=pltpu.VMEM),
        scratch_shapes=[
            pltpu.VMEM((count, rows, a.shape[0]), F32),
            pltpu.SemaphoreType.DMA((count,)),
            pltpu.SemaphoreType.DMA((count,)),
        ],
        compiler_params=pltpu.CompilerParams(
            collective_id=0, has_side_effects=True, vmem_limit_bytes=8 * 1024 * 1024
        ),
        cost_estimate=pl.CostEstimate(
            flops=40_000_000, bytes_accessed=300_000, transcendentals=0
        ),
    )(pair)


def shards(
    layer_input,
    norm_gain,
    in_weights,
    conv_weight,
    conv_bias,
    gate_weights,
    gate_bias,
    decay_rate,
    out_weight,
    mlp_gain,
    mlp_in,
    mlp_out,
):
    rows, own_width = layer_input.shape
    seq_count = lax.axis_size("seq")
    size = square_size(seq_count)
    far = seq_count // size
    seq_here = lax.axis_index("seq")
    place = seq_here % size
    tensor_here = lax.axis_index("tensor")

    halves = mlp_in.shape[0]
    feed = [gather_far(mlp_in[half], 0) for half in range(halves)]
    down_w = gather_far(mlp_out, 1)

    blocks = gather_tensor(layer_input)
    whole = jnp.concatenate(blocks, axis=1)
    values = whole.astype(F32)
    scale = lax.rsqrt(jnp.mean(values * values, axis=-1, keepdims=True) + 1e-06)
    normed = (values * scale * norm_gain).astype(BF16)
    branch_x = jnp.dot(normed, in_weights[0], preferred_element_type=F32).astype(BF16)
    rim_rows = 8
    rim = shifted(branch_x[rows - rim_rows :], "seq", 1)
    branch_y = jax.nn.gelu(
        jnp.dot(normed, in_weights[1], preferred_element_type=F32), approximate=True
    )
    cum_decay, cum_state = recurrence(
        branch_x, rim, conv_weight, conv_bias, gate_weights, gate_bias, decay_rate
    )
    carried = entering_state(cum_decay[-1], cum_state[-1])
    mixed = ((cum_decay * carried + cum_state) * branch_y).astype(BF16)
    partial = jnp.dot(mixed, out_weight, preferred_element_type=F32).astype(BF16)
    residual = (layer_input.astype(F32) + scatter_tensor(partial)).astype(BF16)
    res = residual.astype(F32)
    own_gain = lax.dynamic_slice_in_dim(mlp_gain, tensor_here * own_width, own_width, 0)
    gained = (res * own_gain).astype(BF16)
    squares = jnp.sum(res * res, axis=-1)
    width_all = mlp_gain.shape[0]

    squares = squares + core_swap(squares)
    chips = lax.axis_size("tensor") // CORES
    squares = squares + sum(chip_shift(squares, k) for k in range(1, chips))
    mlp_scale = lax.rsqrt(squares / width_all + 1e-06)[:, None]

    piece = width_all // seq_count
    short = size == 4 and far == CORES and lax.axis_size("tensor") == CORES * CORES
    short = short and own_width == 2 * piece
    offsets = list(range(size - 1, -1, -1))
    if short:
        low, high = spread_columns(gained, piece)
        tokens = {
            o: jnp.concatenate(
                [low[o * rows : (o + 1) * rows], high[o * rows : (o + 1) * rows]], axis=1
            )
            for o in offsets
        }
    else:
        mids = jnp.concatenate(gather_tensor(gained), axis=1)
        wide = mids.reshape(rows, far, size, piece)

        def columns_for(where):
            return lax.dynamic_index_in_dim(wide, where, 2, keepdims=False).reshape(
                rows, far * piece
            )

        tokens = {o: square_swap(columns_for(place ^ o), o) for o in offsets}
    gate_up = []
    for half in range(halves):
        total = jnp.zeros((rows, mlp_in.shape[2]), F32)
        for o in offsets:
            term = jnp.dot(tokens[o], feed[half], preferred_element_type=F32)
            if o:
                term = square_swap(term.astype(BF16), o).astype(F32)
            total = total + term
        gate_up.append(total)
    gate = gate_up[0] * mlp_scale
    hidden = (jax.nn.gelu(gate, approximate=True) * (gate_up[1] * mlp_scale)).astype(BF16)

    spread = {o: square_swap(hidden, o) for o in offsets}
    if short:
        terms = jnp.concatenate(
            [jnp.dot(spread[o], down_w, preferred_element_type=F32) for o in range(size)], axis=0
        )
        return (res + collect_columns(terms, piece).astype(F32)).astype(BF16)
    back = {}
    for o in offsets:
        term = jnp.dot(spread[o], down_w, preferred_element_type=F32)
        back[o] = square_swap(term.astype(BF16), o)
    stacked = jnp.stack([back[o] for o in range(size)])
    ordered = [pick(stacked, place ^ r) for r in range(size)]
    down = jnp.concatenate(
        [ordered[r][:, q * piece : (q + 1) * piece] for q in range(far) for r in range(size)],
        axis=1,
    )
    return (res + scatter_tensor(down)).astype(BF16)


def solution(mesh):
    return jax.shard_map(
        shards,
        mesh=mesh,
        in_specs=(
            P("seq", "tensor"),
            P(),
            P(None, None, "tensor"),
            P(None, "tensor"),
            P("tensor"),
            P(None, "tensor", None, None),
            P(None, "tensor"),
            P("tensor"),
            P("tensor", None),
            P(),
            P(None, "seq", "tensor"),
            P("tensor", "seq"),
        ),
        out_specs=P("seq", "tensor"),
        check_vma=False,
    )
```
